32 devices in a mesh: grp: 2 (over y), bank: 4 (over z), seg: 4 (over x, core).
Axes of the slice: x: 2, y: 2, z: 4, core: 2. Of those that a mesh axis runs over, the one named last changes fastest.
Arguments:
- strain: bfloat16 [32, 2, 32768], P(('grp', 'seg'), None, 'bank'), parts along dimension 0, may hold values from -6 to 6
- templates: bfloat16 [4, 2, 32768], P('bank'), may hold values from -6 to 6
- length_bins: int32 [4], P('bank'), may hold values from 0 to 3
Outputs:
- snr_table: float32 [4, 32], P('bank', ('grp', 'seg')), parts along dimension 1
- segment_peak: float32 [32], P(('grp', 'seg')), parts along dimension 0
- template_peak: float32 [8], P(('grp', 'bank')), parts along dimension 0
The draws below stay inside these ranges and needn't reach their ends.
There are 2 independent parts, one for each index of `grp`. The reference program is written for one: setup_inputs(seed, part) draws one part's arguments, and reference() takes and returns one part's arrays. A program takes and returns all parts, laid end to end along the dimension named above; an argument that names none is the same for every part. Nothing has to cross between parts.
All inputs are finite; a program needn't handle non-finite values.
Results may differ from the reference program's by a relative error of at most 0.0003.
Values may be sent and summed in bfloat16 or wider, within the bound.
No kernel may reach another device: no remote copies, remote signals or barrier semaphores. Data moves between devices by JAX's collectives and lax.ppermute only.
A program may use at most 64 MiB of HBM per device.

```python
import jax
import jax.numpy as jnp
from jax import lax

LEN = 32768
TEMPLATES = 4
SEGMENTS = 16


def with_ends(result, stream_key, least, largest):
    longest = result.shape.index(max(result.shape))
    spots = []
    for shift in (0, 1):
        where = [jax.random.randint(jax.random.fold_in(stream_key, axis), (), 0, length) for axis, length in enumerate(result.shape)]
        where[longest] = (where[longest] + shift) % result.shape[longest]
        spots.append(tuple(where))
    return result.at[spots[0]].set(least).at[spots[1]].set(largest)


def block_scale(rng, shape, pieces, low, largest):
    level, own = 1.0, jax.random.fold_in(rng, 6)
    for axis_at, blocks in pieces:
        draws = jnp.exp(jax.random.uniform(jax.random.fold_in(own, axis_at), (blocks,), jnp.float32, low / len(pieces), largest / len(pieces)))
        level = level * jnp.repeat(draws, shape[axis_at] // blocks).reshape([-1 if axis == axis_at else 1 for axis in range(len(shape))])
    return level


def noise(stream_key, extent, scale, most, split=(), kind=jnp.bfloat16):
    entries = jax.random.normal(stream_key, extent, jnp.float32) * scale
    if len(split) > 0:
        entries = block_scale(stream_key, extent, split, -0.22, 0.18) * entries
    return jnp.clip(entries, min=-most, max=most).astype(kind)


def setup_inputs(seed: int = 0, part: int = 0) -> dict:
    splits = jax.random.split(jax.random.key(seed), 4)
    part_keys = jax.random.split(jax.random.fold_in(splits[3], part), 4)
    strain = noise(part_keys[0], (SEGMENTS, 2, LEN), 1.0, 6.0, ((0, 4), (2, 4)))
    templates = noise(splits[1], (TEMPLATES, 2, LEN), 1.0, 6.0, ((0, 4),))
    length_bins = with_ends(jax.random.randint(splits[2], (TEMPLATES,), 0, 4), jax.random.fold_in(splits[2], 1), 0, 3).astype(jnp.int32)
    return {"strain": strain, "templates": templates, "length_bins": length_bins}


EPSILON = 1e-06

def reference(strain, templates, length_bins):
    seg_real = strain[:, 0, :].astype(jnp.float32)
    seg_imag = strain[:, 1, :].astype(jnp.float32)
    positions = jnp.arange(LEN, dtype=jnp.int32)

    def one_template(inputs):
        template, length_bin = inputs
        cutoff = jnp.right_shift(jnp.int32(LEN), length_bin.astype(jnp.int32))
        keep_mask = positions < cutoff
        tpl_real = jnp.where(keep_mask, template[0].astype(jnp.float32), 0.0)
        tpl_imag = jnp.where(keep_mask, template[1].astype(jnp.float32), 0.0)
        norm_value = jnp.sqrt(jnp.sum(tpl_real * tpl_real + tpl_imag * tpl_imag) + EPSILON)
        prod_real = tpl_real * seg_real + tpl_imag * seg_imag
        prod_imag = tpl_real * seg_imag - tpl_imag * seg_real
        series = jnp.fft.ifft(prod_real + 1j * prod_imag, axis=-1) * LEN
        peak_power = lax.optimization_barrier(jnp.max(jnp.real(series) ** 2 + jnp.imag(series) ** 2, axis=-1))
        return jnp.sqrt(peak_power) / norm_value
    snr_table = lax.map(one_template, (templates, length_bins))
    return (snr_table, lax.optimization_barrier(jnp.max(snr_table, axis=0)), lax.optimization_barrier(jnp.max(snr_table, axis=1)))
```

```python
import functools

import jax
import jax.numpy as jnp
import numpy as np
from jax import lax
from jax.experimental import pallas as pl
from jax.experimental.pallas import tpu as pltpu
from jax.sharding import PartitionSpec as P

EPSILON = 1e-06
LANES = 128


def split_bf16(values):
    high = values.astype(jnp.bfloat16)
    low = (values - high.astype(jnp.float32)).astype(jnp.bfloat16)
    return high, low


def dft_tables(rows):
    row = np.arange(rows)
    lane = np.arange(LANES)
    first = np.exp(2j * np.pi * (np.outer(row, row) % rows) / rows)
    last = np.exp(2j * np.pi * (np.outer(lane, lane) % LANES) / LANES)
    twist = np.exp(2j * np.pi * np.outer(row, lane) / (rows * LANES))
    first = np.block([[first.real, -first.imag], [first.imag, first.real]])
    last = np.block([[last.real, last.imag], [-last.imag, last.real]])
    halves = []
    for table in (first, last):
        table = table.astype(np.float32)
        high = table.astype(jnp.bfloat16)
        halves += [high, (table - high.astype(np.float32)).astype(jnp.bfloat16)]
    return halves + [twist.real.astype(np.float32), twist.imag.astype(np.float32)]


def dot(left, right):
    return jnp.dot(left, right, preferred_element_type=jnp.float32)


def peaks_kernel(
    rows, slab, segs, slabs, tpls, spots, *refs
):
    strain_refs, refs = refs[:slabs], refs[slabs:]
    tpl_refs, refs = refs[:tpls], refs[tpls:]
    first_h, first_l, last_h, last_l, twist_r, twist_i, out_ref = refs[:7]
    prod_h, prod_l, mid, turned_h, turned_l = refs[7:]
    for at in range(slabs):
        spot = pl.multiple_of(spots[at] * slab, slab)
        for t in range(tpls):
            tpl_r = tpl_refs[t][pl.ds(spot, slab), :].astype(jnp.float32)
            tpl_i = tpl_refs[t][pl.ds(rows + spot, slab), :].astype(jnp.float32)
            for s in range(segs):
                base = 2 * s * slab
                seg_r = strain_refs[at][base : base + slab, :].astype(jnp.float32)
                seg_i = strain_refs[at][base + slab : base + 2 * slab, :].astype(jnp.float32)
                f = t * segs + s
                cols = slice(f * LANES, (f + 1) * LANES)
                high, low = split_bf16(tpl_r * seg_r + tpl_i * seg_i)
                prod_h[pl.ds(spot, slab), cols] = high
                prod_l[pl.ds(spot, slab), cols] = low
                high, low = split_bf16(tpl_r * seg_i - tpl_i * seg_r)
                prod_h[pl.ds(rows + spot, slab), cols] = high
                prod_l[pl.ds(rows + spot, slab), cols] = low
    mid[...] = (
        dot(first_h[...], prod_h[...]) + dot(first_h[...], prod_l[...]) + dot(first_l[...], prod_h[...])
    )
    for f in range(tpls * segs):
        cols = slice(f * LANES, (f + 1) * LANES)
        band = slice(f * rows, (f + 1) * rows)
        mid_r, mid_i = mid[:rows, cols], mid[rows:, cols]
        high, low = split_bf16(mid_r * twist_r[...] - mid_i * twist_i[...])
        turned_h[band, :LANES] = high
        turned_l[band, :LANES] = low
        high, low = split_bf16(mid_r * twist_i[...] + mid_i * twist_r[...])
        turned_h[band, LANES:] = high
        turned_l[band, LANES:] = low
    for t in range(tpls):
        tpl = tpl_refs[t][...].astype(jnp.float32)
        sigma = jnp.sqrt(jnp.sum(tpl * tpl, keepdims=True) + EPSILON)
        for s in range(segs):
            f = t * segs + s
            band = slice(f * rows, (f + 1) * rows)
            series = (
                dot(turned_h[band, :], last_h[...])
                + dot(turned_l[band, :], last_h[...])
                + dot(turned_h[band, :], last_l[...])
            )
            series_r, series_i = series[:, :LANES], series[:, LANES:]
            power = jnp.max(series_r * series_r + series_i * series_i, keepdims=True)
            out_ref[f : f + 1, :] = jnp.broadcast_to(jnp.sqrt(power) / sigma, (1, LANES))


def peaks(strains, tpls, spots, rows, segs):
    slab = strains[0].shape[0] // (2 * segs)
    count = segs * len(tpls)

    def body(spots_ref, *refs):
        own = [spots_ref[i] for i in range(len(strains))]
        peaks_kernel(rows, slab, segs, len(strains), len(tpls), own, *refs)

    vmem = pl.BlockSpec(memory_space=pltpu.VMEM)
    tables = [jnp.asarray(t) for t in dft_tables(rows)]
    return pl.pallas_call(
        body,
        name="peaks",
        out_shape=jax.ShapeDtypeStruct((max(8, count), LANES), jnp.float32),
        in_specs=[pl.BlockSpec(memory_space=pltpu.SMEM)]
        + [vmem] * (len(strains) + len(tpls) + len(tables)),
        out_specs=vmem,
        scratch_shapes=[
            pltpu.VMEM((2 * rows, count * LANES), jnp.bfloat16),
            pltpu.VMEM((2 * rows, count * LANES), jnp.bfloat16),
            pltpu.VMEM((2 * rows, count * LANES), jnp.float32),
            pltpu.VMEM((count * rows, 2 * LANES), jnp.bfloat16),
            pltpu.VMEM((count * rows, 2 * LANES), jnp.bfloat16),
        ],
        compiler_params=pltpu.CompilerParams(vmem_limit_bytes=24 * 1024 * 1024),
        cost_estimate=pl.CostEstimate(
            flops=12 * count * (2 * rows) * LANES * (2 * rows + 2 * LANES) // 2,
            bytes_accessed=4 * 1024 * 1024,
            transcendentals=0,
        ),
    )(spots, *strains, *tpls, *tables)


def swap(block, axis, bits):
    return lax.ppermute(block, axis, [(i, i ^ bits) for i in range(lax.axis_size(axis))])


def masked_template(templates, length_bins):
    length = templates.shape[2]
    cutoffs = jnp.right_shift(jnp.int32(length), length_bins)
    keep = jnp.arange(length, dtype=jnp.int32)[None, None, :] < cutoffs[:, None, None]
    return jnp.where(keep, templates, jnp.bfloat16(0))


def paired(strain, templates, length_bins):
    segs, _, width = strain.shape
    length = templates.shape[2]
    rows, slab, half = length // LANES, width // LANES, segs // 2
    z = lax.axis_index("bank")
    side = z & 1
    core = lax.axis_index("seg") & 1
    blocks = strain.reshape(2, 2 * half * slab, LANES)
    mine = lax.dynamic_index_in_dim(blocks, side, 0, False)
    other = lax.dynamic_index_in_dim(blocks, 1 - side, 0, False)
    own_tpl = masked_template(templates, length_bins).reshape(2, rows, LANES)
    part = lax.dynamic_index_in_dim(own_tpl, core, 0, False)
    from_1 = swap(jnp.concatenate([other, part], axis=0), "bank", 1)
    from_2 = swap(mine, "bank", 2)
    from_3 = swap(other, "bank", 3)
    part_a = from_1[2 * half * slab :]
    part_b = swap(part_a, "seg", 1)
    pair_tpl = jnp.where(
        core == 0, jnp.concatenate([part_a, part_b]), jnp.concatenate([part_b, part_a])
    )
    spots = jnp.stack([z, z ^ 1, z ^ 2, z ^ 3]).astype(jnp.int32)
    table = peaks(
        [mine, from_1[: 2 * half * slab], from_2, from_3],
        [own_tpl.reshape(2 * rows, LANES), pair_tpl],
        spots, rows, half,
    )[: 2 * half]
    there = swap(table, "bank", 1)
    own_row = jnp.stack([table[:half], there[half:]])
    pair_row = jnp.stack([table[half:], there[:half]])
    seg_peak = jnp.maximum(own_row, pair_row)
    tpl_peak = jnp.max(own_row, axis=(0, 1))[None]
    tpl_peak = jnp.maximum(tpl_peak, swap(tpl_peak, "seg", 1))
    seg_peak = jnp.maximum(seg_peak, swap(seg_peak, "bank", 2))
    step = 2
    while step < lax.axis_size("seg"):
        tpl_peak = jnp.maximum(tpl_peak, swap(tpl_peak, "seg", step))
        step *= 2

    def ordered(pair):
        pair = pair[:, :, 0]
        return jnp.where(side == 0, pair, pair[::-1]).reshape(segs)

    return ordered(own_row)[None], ordered(seg_peak), tpl_peak[:, 0]


def gathered(strain, templates, length_bins):
    segs = strain.shape[0]
    tpls, _, length = templates.shape
    rows = length // LANES
    whole = lax.all_gather(strain, "bank", axis=2, tiled=True).reshape(segs * 2 * rows, LANES)
    own = masked_template(templates, length_bins).reshape(tpls, 2 * rows, LANES)
    spots = jnp.zeros((1,), jnp.int32)
    lists = [peaks([whole], [own[t]], spots, rows, segs)[:segs, 0] for t in range(tpls)]
    table = jnp.stack(lists)
    seg_peak = lax.pmax(jnp.max(table, axis=0), "bank")
    tpl_peak = lax.pmax(jnp.max(table, axis=1), "seg")
    return table, seg_peak, tpl_peak


def per_device(strain, templates, length_bins):
    banks, segs_size = lax.axis_size("bank"), lax.axis_size("seg")
    fits = (
        banks == 4
        and segs_size >= 2
        and segs_size & (segs_size - 1) == 0
        and templates.shape[0] == 1
        and strain.shape[0] % 2 == 0
        and strain.shape[2] % (16 * LANES) == 0
    )
    return (paired if fits else gathered)(strain, templates, length_bins)


def solution(mesh):
    placed = (P(("grp", "seg"), None, "bank"), P("bank", None, None), P("bank"))
    return jax.shard_map(
        per_device,
        mesh=mesh,
        in_specs=placed,
        out_specs=(P("bank", ("grp", "seg")), P(("grp", "seg")), P(("grp", "bank"))),
        check_vma=False,
    )
```

```python
import jax
import jax.numpy as jnp
import numpy as np
from jax import lax
from jax.experimental import pallas as pl
from jax.experimental.pallas import tpu as pltpu
from jax.sharding import PartitionSpec as P


EPSILON = 1e-06
LANES = 128
VMEM_BYTES = 24 * 1024 * 1024


def split_bf16(values):
    high = values.astype(jnp.bfloat16)
    low = (values - high.astype(jnp.float32)).astype(jnp.bfloat16)
    return high, low


def halves(table):
    table = table.astype(np.float32)
    high = table.astype(jnp.bfloat16)
    return [high, (table - high.astype(np.float32)).astype(jnp.bfloat16)]


def dft_tables(rows):
    row = np.arange(rows)
    lane = np.arange(LANES)
    first = np.exp(2j * np.pi * (np.outer(row, row) % rows) / rows)
    last = np.exp(2j * np.pi * (np.outer(lane, lane) % LANES) / LANES)
    twist = np.exp(2j * np.pi * np.outer(row, lane) / (rows * LANES))
    first = np.stack(
        [
            np.block([[part.real, -part.imag], [part.imag, part.real]])
            for part in np.split(first, 2, axis=1)
        ]
    )
    last = np.block([[last.real, last.imag], [-last.imag, last.real]])
    twists = [twist.real.astype(np.float32), twist.imag.astype(np.float32)]
    return halves(first), halves(last) + twists


def dot(left, right):
    return jnp.dot(left, right, preferred_element_type=jnp.float32)


def fill(strain, stride, base, count, tpls, tpl_at, segs, prods, at):
    prod_h, prod_l = prods
    rows, depth = tpls[0].shape[0] // 2, prod_h.shape[0] // 2
    for t, tpl in enumerate(tpls):
        tpl_r = tpl[pl.ds(tpl_at, count), :].astype(jnp.float32)
        tpl_i = tpl[pl.ds(rows + tpl_at, count), :].astype(jnp.float32)
        for s in range(segs):
            at_r, at_i = 2 * s * stride + base, (2 * s + 1) * stride + base
            seg_r = strain[at_r : at_r + count, :].astype(jnp.float32)
            seg_i = strain[at_i : at_i + count, :].astype(jnp.float32)
            cols = slice((t * segs + s) * LANES, (t * segs + s + 1) * LANES)
            high, low = split_bf16(tpl_r * seg_r + tpl_i * seg_i)
            prod_h[pl.ds(at, count), cols] = high
            prod_l[pl.ds(at, count), cols] = low
            high, low = split_bf16(tpl_r * seg_i - tpl_i * seg_r)
            prod_h[pl.ds(depth + at, count), cols] = high
            prod_l[pl.ds(depth + at, count), cols] = low


def begin_kernel(pieces, half_of, segs, n_tpls, *refs):
    n_strains = len(pieces)
    strains, refs = refs[:n_strains], refs[n_strains:]
    tpls, refs = refs[:n_tpls], refs[n_tpls:]
    first_h, first_l, mid_ref, sigma_ref, prod_h, prod_l = refs
    for piece, strain in zip(pieces, strains):
        stride, base, count, tpl_at, at = piece()
        fill(strain, stride, base, count, tpls, tpl_at, segs, (prod_h, prod_l), at)
    half = half_of()
    mid_ref[...] = (
        dot(first_h[half], prod_h[...])
        + dot(first_h[half], prod_l[...])
        + dot(first_l[half], prod_h[...])
    )
    for t, tpl_ref in enumerate(tpls):
        tpl = tpl_ref[...].astype(jnp.float32)
        sigma = jnp.sqrt(jnp.sum(tpl * tpl, keepdims=True) + EPSILON)
        for f in range(t * segs, (t + 1) * segs):
            sigma_ref[f : f + 1, :] = jnp.broadcast_to(sigma, (1, LANES))


def end_kernel(pieces, half_of, row_of, segs, n_tpls, *refs):
    n_strains = len(pieces)
    strains, refs = refs[:n_strains], refs[n_strains:]
    tpls, refs = refs[:n_tpls], refs[n_tpls:]
    first_h, first_l, last_h, last_l, twist_r, twist_i, mid_ref, sigma_ref, out_ref = refs[:9]
    prod_h, prod_l, total, turned_h, turned_l = refs[9:]
    rows = twist_r.shape[0]
    out_ref[...] = jnp.zeros_like(out_ref)
    for piece, strain in zip(pieces, strains):
        stride, base, count, tpl_at, at = piece()
        fill(strain, stride, base, count, tpls, tpl_at, segs, (prod_h, prod_l), at)
    half = half_of()
    total[...] = (
        dot(first_h[half], prod_h[...])
        + dot(first_h[half], prod_l[...])
        + dot(first_l[half], prod_h[...])
    )
    for f in range(n_tpls * segs):
        cols = slice(f * LANES, (f + 1) * LANES)
        band = slice(f * rows, (f + 1) * rows)
        mid_r = total[:rows, cols] + mid_ref[:rows, cols]
        mid_i = total[rows:, cols] + mid_ref[rows:, cols]
        high, low = split_bf16(mid_r * twist_r[...] - mid_i * twist_i[...])
        turned_h[band, :LANES] = high
        turned_l[band, :LANES] = low
        high, low = split_bf16(mid_r * twist_i[...] + mid_i * twist_r[...])
        turned_h[band, LANES:] = high
        turned_l[band, LANES:] = low
    for f in range(n_tpls * segs):
        band = slice(f * rows, (f + 1) * rows)
        series = (
            dot(turned_h[band, :], last_h[...])
            + dot(turned_l[band, :], last_h[...])
            + dot(turned_h[band, :], last_l[...])
        )
        series_r, series_i = series[:, :LANES], series[:, LANES:]
        power = jnp.max(series_r * series_r + series_i * series_i, keepdims=True)
        row = row_of(f // segs, f % segs)
        out_ref[pl.ds(row, 1), :] = jnp.sqrt(power) / sigma_ref[f : f + 1, :]


def vmem_specs(count):
    return [pl.BlockSpec(memory_space=pltpu.VMEM)] * count


def begin(strains, pieces, half_of, tpls, first, rows, segs):
    count = segs * len(tpls)
    return pl.pallas_call(
        lambda *refs: begin_kernel(pieces, half_of, segs, len(tpls), *refs),
        name="begin",
        out_shape=[
            jax.ShapeDtypeStruct((2 * rows, count * LANES), jnp.float32),
            jax.ShapeDtypeStruct((max(8, count), LANES), jnp.float32),
        ],
        in_specs=vmem_specs(len(strains) + len(tpls) + 2),
        out_specs=vmem_specs(2),
        scratch_shapes=[pltpu.VMEM((rows, count * LANES), jnp.bfloat16)] * 2,
        compiler_params=pltpu.CompilerParams(vmem_limit_bytes=VMEM_BYTES),
        cost_estimate=pl.CostEstimate(
            flops=6 * count * 2 * rows * rows * LANES,
            bytes_accessed=2 * 1024 * 1024,
            transcendentals=0,
        ),
    )(*strains, *tpls, *first)


def end(strains, pieces, half_of, row_of, out_rows, tpls, first, rest, mid, sigma, rows, segs):
    count = segs * len(tpls)
    return pl.pallas_call(
        lambda *refs: end_kernel(pieces, half_of, row_of, segs, len(tpls), *refs),
        name="end",
        out_shape=jax.ShapeDtypeStruct((out_rows, LANES), jnp.float32),
        in_specs=vmem_specs(len(strains) + len(tpls) + len(first) + len(rest) + 2),
        out_specs=pl.BlockSpec(memory_space=pltpu.VMEM),
        scratch_shapes=[
            pltpu.VMEM((rows, count * LANES), jnp.bfloat16),
            pltpu.VMEM((rows, count * LANES), jnp.bfloat16),
            pltpu.VMEM((2 * rows, count * LANES), jnp.float32),
            pltpu.VMEM((count * rows, 2 * LANES), jnp.bfloat16),
            pltpu.VMEM((count * rows, 2 * LANES), jnp.bfloat16),
        ],
        compiler_params=pltpu.CompilerParams(vmem_limit_bytes=VMEM_BYTES),
        cost_estimate=pl.CostEstimate(
            flops=6 * count * 2 * rows * (rows + 2 * LANES) * LANES,
            bytes_accessed=4 * 1024 * 1024,
            transcendentals=0,
        ),
    )(*strains, *tpls, *first, *rest, mid, sigma)


def cutoff_kernel(length, bins_ref, cut_ref):
    cut_ref[...] = jnp.full(cut_ref.shape, jnp.right_shift(jnp.int32(length), bins_ref[0]), jnp.int32)


def cutoff(length, length_bins):
    return pl.pallas_call(
        lambda *refs: cutoff_kernel(length, *refs),
        name="cutoff",
        out_shape=jax.ShapeDtypeStruct((8, LANES), jnp.int32),
        in_specs=[pl.BlockSpec(memory_space=pltpu.SMEM)],
        out_specs=pl.BlockSpec(memory_space=pltpu.VMEM),
        compiler_params=pltpu.CompilerParams(vmem_limit_bytes=VMEM_BYTES),
        cost_estimate=pl.CostEstimate(flops=10**6, bytes_accessed=2**22, transcendentals=0),
    )(length_bins)


def mask_kernel(cut_ref, tpl_ref, other_ref, own_ref, sent_ref):
    rows = tpl_ref.shape[0] // 2
    height = other_ref.shape[0]
    place = lax.broadcasted_iota(jnp.int32, (rows, LANES), 0) * LANES
    place = place + lax.broadcasted_iota(jnp.int32, (rows, LANES), 1)
    keep = place < cut_ref[:1, :]
    core = lax.axis_index("seg") & 1
    for part in range(2):
        values = tpl_ref[part * rows : (part + 1) * rows, :].astype(jnp.float32)
        own_ref[part * rows : (part + 1) * rows, :] = jnp.where(keep, values, 0.0).astype(jnp.bfloat16)
    sent_ref[:height, :] = other_ref[...]
    sent_ref[height:, :] = own_ref[pl.ds(pl.multiple_of(core * rows, rows), rows), :]


def last_kernel(own_ref, seg_ref, seg_there_ref, tpl_ref, tpl_there_ref, snr_out, seg_out, tpl_out):
    segs = own_ref.shape[0]
    lane = lax.broadcasted_iota(jnp.int32, (1, LANES), 1)

    def across(block):
        line = block[:1, :]
        for i in range(1, segs):
            line = jnp.where(lane == i, block[i : i + 1, :], line)
        return line[:, :segs]

    snr_out[...] = across(own_ref[...])
    seg_out[...] = across(jnp.maximum(seg_ref[...], seg_there_ref[...]))
    tpl_out[...] = jnp.maximum(tpl_ref[...], tpl_there_ref[...])[:, :1]


def swap(block, axis, bits):
    return lax.ppermute(block, axis, [(i, i ^ bits) for i in range(lax.axis_size(axis))])


def paired(strain, templates, length_bins):
    segs, _, width = strain.shape
    length = templates.shape[2]
    rows, slab, half = length // LANES, width // LANES, segs // 2
    z = lax.axis_index("bank")
    side = z & 1
    core = lax.axis_index("seg") & 1
    height = 2 * half * slab
    first, rest = ([jnp.asarray(t) for t in part] for part in dft_tables(rows))
    cut = cutoff(length, length_bins)
    pass
    blocks = strain.reshape(2, height, LANES)
    mine = lax.dynamic_index_in_dim(blocks, side, 0, False)
    other = lax.dynamic_index_in_dim(blocks, 1 - side, 0, False)
    own_tpl, sent = pl.pallas_call(
        mask_kernel,
        name="mask",
        out_shape=[
            jax.ShapeDtypeStruct((2 * rows, LANES), jnp.bfloat16),
            jax.ShapeDtypeStruct((height + rows, LANES), jnp.bfloat16),
        ],
        in_specs=vmem_specs(3),
        out_specs=vmem_specs(2),
        compiler_params=pltpu.CompilerParams(vmem_limit_bytes=VMEM_BYTES),
    )(cut, templates.reshape(2 * rows, LANES), other)
    from_1 = swap(sent, "bank", 1)
    from_2 = swap(mine, "bank", 2)
    from_3 = swap(other, "bank", 3)
    part_a = from_1[height:]
    part_b = swap(part_a, "seg", 1)
    pair_tpl = jnp.where(
        core == 0, jnp.concatenate([part_a, part_b]), jnp.concatenate([part_b, part_a])
    )
    tpls = [own_tpl, pair_tpl]

    def piece(bits):
        def place():
            bank = lax.axis_index("bank") ^ bits
            at = pl.multiple_of((bank & 1) * slab, slab)
            return slab, 0, slab, pl.multiple_of(bank * slab, slab), at

        return place

    mid, sigma = begin(
        [mine, from_1[:height]], [piece(0), piece(1)],
        lambda: lax.axis_index("bank") >> 1, tpls, first, rows, half,
    )

    def row_of(t, s):
        side = lax.axis_index("bank") & 1
        return (side ^ t) * segs + side * half + s

    table = end(
        [from_2, from_3], [piece(2), piece(3)],
        lambda: 1 - (lax.axis_index("bank") >> 1), row_of, 2 * segs,
        tpls, first, rest, mid, sigma, rows, half,
    )
    table = jnp.maximum(table, swap(table, "bank", 1))
    own_row = lax.dynamic_slice_in_dim(table, side * segs, segs, 0)
    tpl_peak = jnp.max(own_row, axis=0, keepdims=True)
    tpl_peak = jnp.maximum(tpl_peak, swap(tpl_peak, "seg", 1))
    seg_peak = jnp.maximum(table[:segs], table[segs:])
    seg_there = swap(seg_peak, "bank", 2)
    step = 2
    while 2 * step < lax.axis_size("seg"):
        tpl_peak = jnp.maximum(tpl_peak, swap(tpl_peak, "seg", step))
        step *= 2
    tpl_there = swap(tpl_peak, "seg", step) if step < lax.axis_size("seg") else tpl_peak
    snr, seg_out, tpl_out = pl.pallas_call(
        last_kernel,
        name="last",
        out_shape=[
            jax.ShapeDtypeStruct((1, segs), jnp.float32),
            jax.ShapeDtypeStruct((1, segs), jnp.float32),
            jax.ShapeDtypeStruct((1, 1), jnp.float32),
        ],
        in_specs=vmem_specs(5),
        out_specs=vmem_specs(3),
        compiler_params=pltpu.CompilerParams(vmem_limit_bytes=VMEM_BYTES),
    )(own_row, seg_peak, seg_there, tpl_peak, tpl_there)
    return snr, seg_out[0], tpl_out[0]


def gathered(strain, templates, length_bins):
    segs = strain.shape[0]
    tpls, _, length = templates.shape
    rows = length // LANES
    deep = rows // 2
    first, rest = ([jnp.asarray(t) for t in part] for part in dft_tables(rows))
    whole = lax.all_gather(strain, "bank", axis=2, tiled=True).reshape(segs * 2 * rows, LANES)
    cutoffs = jnp.right_shift(jnp.int32(length), length_bins)
    keep = jnp.arange(length, dtype=jnp.int32)[None, None, :] < cutoffs[:, None, None]
    own = jnp.where(keep, templates, jnp.bfloat16(0)).reshape(tpls, 2 * rows, LANES)
    lists = []
    for t in range(tpls):
        mid, sigma = begin(
            [whole], [lambda: (rows, 0, deep, 0, 0)], lambda: 0, [own[t]], first, rows, segs
        )
        table = end(
            [whole], [lambda: (rows, deep, deep, deep, 0)], lambda: 1,
            lambda t, s: s, segs, [own[t]], first, rest, mid, sigma, rows, segs,
        )
        lists.append(table[:segs, 0])
    table = jnp.stack(lists)
    seg_peak = lax.pmax(jnp.max(table, axis=0), "bank")
    tpl_peak = lax.pmax(jnp.max(table, axis=1), "seg")
    return table, seg_peak, tpl_peak


def pairs_fit(mesh, strain, templates):
    banks, columns = mesh.shape["bank"], mesh.shape["seg"]
    segs = strain.shape[0] // (mesh.shape["grp"] * columns)
    return (
        banks == 4
        and columns >= 2
        and columns & (columns - 1) == 0
        and templates.shape[0] == banks
        and segs % 2 == 0
        and strain.shape[2] % (16 * LANES * banks) == 0
    )


def solution(mesh):
    placed = (P(("grp", "seg"), None, "bank"), P("bank", None, None), P("bank"))

    def whole(strain, templates, length_bins):
        fits = pairs_fit(mesh, strain, templates)

        def per_device(*args):
            return (paired if fits else gathered)(*args)

        return jax.shard_map(
            per_device,
            mesh=mesh,
            in_specs=placed,
            out_specs=(P("bank", ("grp", "seg")), P(("grp", "seg")), P(("grp", "bank"))),
            check_vma=False,
        )(strain, templates, length_bins)

    return whole
```
